256 devices in a mesh: dp: 64 (over z, x, core), tensor: 4 (over y).
Axes of the slice: x: 4, y: 4, z: 8, core: 2. Of those that a mesh axis runs over, the one named last changes fastest.
Arguments:
- queries: bfloat16 [2048, 32, 2048], P('dp', None, 'tensor'), may hold values from -8 to 8
- keys: bfloat16 [2048, 32, 512], P('dp', None, 'tensor'), may hold values from -8 to 8
- values: bfloat16 [2048, 32, 512], P('dp', None, 'tensor'), may hold values from -6 to 6
- out_weight: bfloat16 [2048, 4096], P(None, 'tensor'), may hold values from -0.125 to 0.125
- dest_slot: int32 [2048], P('dp'), may hold values from 0 to 63, as said below
- pack_slot: int32 [64, 32], P('dp'), may hold values from 0 to 63, as said below
- seq_start: int32 [64, 32], P('dp'), may hold values from 0 to 1024, as said below
- seq_len: int32 [64, 32], P('dp'), may hold values from 0 to 1024, as said below
Outputs:
- projected: bfloat16 [2048, 32, 4096], P('dp', None, 'tensor')
The draws below stay inside these ranges and needn't reach their ends.
Inputs may be any that keep to these rules, and one draw needn't show every extreme that they name: Block i of loader l goes to pack dest_slot[l * 32 + i]; the 32 values of one loader are distinct. pack_slot[p, s] = l + m names the block of loader l whose dest_slot is p + m; the values of one pack are distinct, and every block of every loader fills exactly one position of one pack, so each pack holds exactly 32 blocks. Multiples of 32; seq_start[p, 0] = 0, the used entries rise, and a sequence's blocks run up to the next used start (or to the pack's end); the entries after the used ones equal 1024. Some pack holds a single sequence of all its blocks. `seq_len`: for a used sequence of b blocks, from b * 32 - 32 // 4 + 1 to b * 32; 0 for unused entries.
All inputs are finite; a program needn't handle non-finite values.
Results may differ from the reference program's by a relative error of at most 0.01.
Values may be sent and summed in bfloat16 or wider, within the bound.
A program may use at most 64 MiB of HBM per device.

```python
import jax
import jax.numpy as jnp
from jax import lax

D = 4096
HEAD_SIZE = 128
QUERY_HEADS = 16
KEY_VALUE_HEADS = 4
BLOCK_ROWS = 32
LOADER_BLOCKS = 32
CAP = 1
TOTAL_BLOCKS = 2048
N_DP = 64


def local_order(sub_key):
    return jax.random.permutation(sub_key, LOADER_BLOCKS)


def routing_tables(key):
    base_key = jax.random.fold_in(key, 7001)
    keys_four = jax.random.split(base_key, 4)
    order_a = jax.random.permutation(keys_four[0], N_DP).astype(jnp.int32)
    order_b = jax.random.permutation(keys_four[1], N_DP).astype(jnp.int32)
    offsets = jax.random.permutation(keys_four[2], N_DP).astype(jnp.int32)
    position = jnp.arange(LOADER_BLOCKS, dtype=jnp.int32)
    shift_of = offsets[position % N_DP]
    layer_of = position // N_DP
    loader_of = order_a[(order_b[:, None] + shift_of[None, :]) % N_DP]
    pack_table = (loader_of * CAP + layer_of[None, :]).astype(jnp.int32)
    inverse_a = jnp.argsort(order_a).astype(jnp.int32)
    inverse_b = jnp.argsort(order_b).astype(jnp.int32)
    pack_of = inverse_b[(inverse_a[:, None] - shift_of[None, :]) % N_DP]
    sending = (pack_of * CAP + layer_of[None, :]).astype(jnp.int32)
    local_orders = jax.vmap(local_order)(jax.random.split(keys_four[3], N_DP)).astype(jnp.int32)
    loader_rows = jnp.arange(N_DP, dtype=jnp.int32)[:, None] * jnp.ones((1, LOADER_BLOCKS), jnp.int32)
    dest_table = jnp.zeros((N_DP, LOADER_BLOCKS), jnp.int32).at[loader_rows, local_orders].set(sending)
    return (dest_table.reshape(TOTAL_BLOCKS), pack_table)


def segment_tables(key):
    base_key = jax.random.fold_in(key, 7002)
    keys_four = jax.random.split(base_key, 4)
    cut_rates = jax.random.randint(keys_four[0], (N_DP,), 0, 9)
    single_pack = jax.random.randint(keys_four[1], (), 0, N_DP)
    cut_rates = jnp.where(jnp.arange(N_DP) == single_pack, 0, cut_rates)
    coin_draws = jax.random.randint(keys_four[2], (N_DP, LOADER_BLOCKS), 0, 8)
    position = jnp.arange(LOADER_BLOCKS, dtype=jnp.int32)
    boundary = (coin_draws < cut_rates[:, None]) | (position[None, :] == 0)
    starts_block = jnp.sort(jnp.where(boundary, position[None, :], LOADER_BLOCKS), axis=1).astype(jnp.int32)
    following = jnp.concatenate([starts_block[:, 1:], jnp.full((N_DP, 1), LOADER_BLOCKS, jnp.int32)], axis=1)
    counts = jnp.where(starts_block < LOADER_BLOCKS, following - starts_block, 0)
    padding = jax.random.randint(keys_four[3], (N_DP, LOADER_BLOCKS), 0, max(BLOCK_ROWS // 4, 1))
    lengths = jnp.where(counts > 0, counts * BLOCK_ROWS - padding, 0).astype(jnp.int32)
    return ((starts_block * BLOCK_ROWS).astype(jnp.int32), lengths)


def draw_dest_slot(key, part):
    return routing_tables(key)[0]


def draw_pack_slot(key, part):
    return routing_tables(key)[1]


def draw_seq_start(key, part):
    return segment_tables(key)[0]


def draw_seq_len(key, part):
    return segment_tables(key)[1]


def draw_queries(key, part):
    noise_key = jax.random.fold_in(key, 7004)
    overall_shape = (TOTAL_BLOCKS, BLOCK_ROWS, QUERY_HEADS * HEAD_SIZE)
    base_draw = jnp.clip(jax.random.normal(noise_key, overall_shape, jnp.float32), -6.0, 6.0)
    return base_draw.astype(jnp.bfloat16)


def draw_keys(key, part):
    noise_key = jax.random.fold_in(key, 7006)
    overall_shape = (TOTAL_BLOCKS, BLOCK_ROWS, KEY_VALUE_HEADS * HEAD_SIZE)
    base_draw = jnp.clip(jax.random.normal(noise_key, overall_shape, jnp.float32), -6.0, 6.0)
    return base_draw.astype(jnp.bfloat16)


def block_levels(key, shape, cuts, low, top_value):
    def one(dim, shards_of):
        draws = jax.random.uniform(jax.random.fold_in(jax.random.fold_in(key, 6), dim), (shards_of,), jnp.float32, low / len(cuts), top_value / len(cuts))
        return jnp.repeat(jnp.exp(draws), shape[dim] // shards_of).reshape((-1,) + (1,) * (len(shape) - dim - 1))

    gain = one(*cuts[0])
    for cut in cuts[1:]:
        gain = gain * one(*cut)
    return gain


def scatter_about(stream_key, shape, scale, most, pieces=(), kind=jnp.bfloat16):
    drawn = jax.random.normal(stream_key, shape, jnp.float32) * scale
    if len(pieces) > 0:
        drawn = block_levels(stream_key, shape, pieces, -0.22, 0.18) * drawn
    return jnp.clip(drawn, min=-most, max=most).astype(kind)


def setup_inputs(seed: int = 0) -> dict:
    key_list = jax.random.split(jax.random.key(seed), 9)
    queries = draw_queries(jax.random.fold_in(key_list[8], 71), 0)
    keys = draw_keys(jax.random.fold_in(key_list[8], 71), 0)
    values = scatter_about(key_list[2], (TOTAL_BLOCKS, BLOCK_ROWS, KEY_VALUE_HEADS * HEAD_SIZE), 1.0, 6.0, ((0, 64), (2, 4)))
    out_weight = scatter_about(key_list[3], (QUERY_HEADS * HEAD_SIZE, D), (QUERY_HEADS * HEAD_SIZE) ** -0.5, 0.125, ((1, 4),))
    dest_slot = draw_dest_slot(jax.random.fold_in(key_list[8], 71), 0)
    pack_slot = draw_pack_slot(jax.random.fold_in(key_list[8], 71), 0)
    seq_start = draw_seq_start(jax.random.fold_in(key_list[8], 71), 0)
    seq_len = draw_seq_len(jax.random.fold_in(key_list[8], 71), 0)
    return {"queries": queries, "keys": keys, "values": values, "out_weight": out_weight, "dest_slot": dest_slot, "pack_slot": pack_slot, "seq_start": seq_start, "seq_len": seq_len}


def pack_attention(packed_queries, packed_keys, packed_values, starts, lengths):
    total_row_count = packed_queries.shape[0]
    query_group_count = QUERY_HEADS // KEY_VALUE_HEADS
    tile_rows = 16 * BLOCK_ROWS
    score_scale = 1.0 / (HEAD_SIZE ** 0.5)
    row_ids = jnp.arange(total_row_count, dtype=jnp.int32)
    segment = (jnp.sum((starts[None, :] <= row_ids[:, None]).astype(jnp.int32), axis=1) - 1).astype(jnp.int32)
    begins = jnp.take(starts, segment)
    limits = jnp.take(lengths, segment)
    usable = (row_ids - begins) < limits
    query_head_rows = packed_queries.astype(jnp.float32).reshape(total_row_count, KEY_VALUE_HEADS, query_group_count, HEAD_SIZE)
    key_head_rows = packed_keys.astype(jnp.float32).reshape(total_row_count, KEY_VALUE_HEADS, HEAD_SIZE)
    value_head_rows = packed_values.astype(jnp.float32).reshape(total_row_count, KEY_VALUE_HEADS, HEAD_SIZE)
    blocks_out = []
    for tile_index in range(total_row_count // tile_rows):
        first_row = tile_index * tile_rows
        end_row = first_row + tile_rows
        scores = jnp.einsum("rgnd,cgd->gnrc", query_head_rows[first_row:end_row], key_head_rows[:end_row]) * score_scale
        allowed = (segment[first_row:end_row, None] == segment[None, :end_row]) & (row_ids[None, :end_row] <= row_ids[first_row:end_row, None])
        scores = jnp.where(allowed[None, None], scores, -jnp.inf)
        largest = jnp.max(scores, axis=-1, keepdims=True)
        exponent = jnp.exp(scores - largest)
        weights = (exponent / jnp.sum(exponent, axis=-1, keepdims=True)).astype(jnp.bfloat16)
        mixture = jnp.einsum("gnrc,cgd->rgnd", weights.astype(jnp.float32), value_head_rows[:end_row])
        mixture = jnp.where(usable[first_row:end_row, None, None, None], mixture, 0.0)
        blocks_out.append(mixture.reshape(tile_rows, QUERY_HEADS * HEAD_SIZE).astype(jnp.bfloat16))
    return jnp.concatenate(blocks_out, axis=0)


def reference(queries, keys, values, out_weight, dest_slot, pack_slot, seq_start, seq_len):
    dest_table = dest_slot.reshape(N_DP, LOADER_BLOCKS)
    positions = jnp.arange(LOADER_BLOCKS, dtype=jnp.int32)

    def one_pack(pack_index):
        slot_row = pack_slot[pack_index]
        loader = (slot_row // CAP).astype(jnp.int32)
        wanted = (pack_index * CAP + slot_row % CAP).astype(jnp.int32)
        candidates = dest_table[loader]
        local_index = jnp.sum(jnp.where(candidates == wanted[:, None], positions[None, :], 0), axis=1)
        source_block = (loader * LOADER_BLOCKS + local_index).astype(jnp.int32)
        attended = pack_attention(
            queries[source_block].reshape(LOADER_BLOCKS * BLOCK_ROWS, QUERY_HEADS * HEAD_SIZE),
            keys[source_block].reshape(LOADER_BLOCKS * BLOCK_ROWS, KEY_VALUE_HEADS * HEAD_SIZE),
            values[source_block].reshape(LOADER_BLOCKS * BLOCK_ROWS, KEY_VALUE_HEADS * HEAD_SIZE),
            seq_start[pack_index],
            seq_len[pack_index],
        )
        return attended.reshape(LOADER_BLOCKS, BLOCK_ROWS, QUERY_HEADS * HEAD_SIZE), source_block

    results, sources = lax.map(one_pack, jnp.arange(N_DP, dtype=jnp.int32))
    at_home = jnp.zeros((TOTAL_BLOCKS, BLOCK_ROWS, QUERY_HEADS * HEAD_SIZE), jnp.bfloat16).at[sources.reshape(-1)].set(results.reshape(TOTAL_BLOCKS, BLOCK_ROWS, QUERY_HEADS * HEAD_SIZE))
    projected = jnp.dot(at_home.reshape(TOTAL_BLOCKS * BLOCK_ROWS, QUERY_HEADS * HEAD_SIZE), out_weight, preferred_element_type=jnp.float32)
    return projected.astype(jnp.bfloat16).reshape(TOTAL_BLOCKS, BLOCK_ROWS, D)
```

```python
import functools

import jax
import jax.numpy as jnp
from jax import lax
from jax.experimental import pallas as pl
from jax.experimental.pallas import tpu as pltpu
from jax.sharding import PartitionSpec as P

MESH = pl.DeviceIdType.MESH
HEAD_SIZE = 128
NZ, NX, NC, NY = 8, 4, 2, 4
BLOCKS, ROWS, COLS = 32, 32, 512
GROUP = 256
HALF = 128
NEG = -1e30
FAR = 1 << 20
LOG2E = 1.4426950408889634


def lookup_tables(dest_slot, pack_slot, seq_start, seq_len):
    mine = jnp.concatenate([dest_slot, pack_slot[0], seq_start[0], seq_len[0]])
    table = lax.all_gather(mine, "dp")
    me = lax.axis_index("dp")
    z, x, c = me // (NX * NC), (me // NC) % NX, me % NC
    count = jnp.arange(BLOCKS, dtype=jnp.int32)
    dest, sources = table[:, :32], table[:, 32:64]
    query_loader = (z * NX + (x + jnp.arange(NX)) % NX) * NC + c
    pack = jnp.take(dest, query_loader, axis=0).reshape(-1)
    rows = jnp.take(table, pack, axis=0)
    loader = jnp.repeat(query_loader, BLOCKS)[:, None]
    place = jnp.sum(jnp.where(rows[:, 32:64] == loader, count, 0), axis=1)
    starts = rows[:, 64:96]
    begin = jnp.max(jnp.where(starts <= place[:, None] * ROWS, starts, 0), axis=1)
    length = jnp.sum(jnp.where(starts == begin[:, None], rows[:, 96:], 0), axis=1)
    left = begin + length - place * ROWS
    key_z = jnp.tile((z + jnp.arange(NZ)) % NZ, NC)
    key_c = jnp.repeat((c + jnp.arange(NC)) % NC, NZ)
    key_loader = (key_z * NX + x) * NC + key_c
    found = sources[:, None, :] == key_loader[None, :, None]
    position = jnp.sum(jnp.where(found, count, 0), axis=2)
    position = jnp.where(jnp.any(found, axis=2), position * ROWS, FAR)
    key_row = (position[:, :, None] + jnp.arange(ROWS, dtype=jnp.int32)).reshape(N_PACKS, NC * NZ * ROWS)
    packs = jnp.arange(N_PACKS, dtype=jnp.int32)
    held = jnp.take(dest, key_loader, axis=0)[None] == packs[:, None, None]
    block = jnp.sum(jnp.where(held, count, 0), axis=2)
    query_table = jnp.concatenate([pack, place, begin, left[:BLOCKS]]).astype(jnp.int32)
    return query_table, block.reshape(-1).astype(jnp.int32), key_row.astype(jnp.int32)


N_PACKS = NZ * NX * NC


def heads_down(tile):
    return jnp.concatenate([tile[:, h * HEAD_SIZE : (h + 1) * HEAD_SIZE] for h in range(4)], axis=0)


def heads_across(tile):
    return jnp.concatenate([tile[h * ROWS : (h + 1) * ROWS] for h in range(4)], axis=1)


def diagonal():
    shape = (HEAD_SIZE, HEAD_SIZE)
    return lax.broadcasted_iota(jnp.int32, shape, 0) == lax.broadcasted_iota(jnp.int32, shape, 1)


def merge(parts):
    top = functools.reduce(jnp.maximum, [s for _, s in parts])
    shares = [jnp.exp2(s - top) for _, s in parts]
    total = functools.reduce(jnp.add, shares)
    shares = [s / total for s in shares]
    eye = diagonal()
    merged = []
    for b in range(4):
        weights = jnp.concatenate(
            [jnp.where(eye, s[b : b + 1], 0.0).astype(jnp.bfloat16) for s in shares], axis=1
        )
        outputs = jnp.concatenate([heads_down(o[b * ROWS : (b + 1) * ROWS]) for o, _ in parts], axis=0)
        merged.append(heads_across(jnp.dot(weights, outputs, preferred_element_type=jnp.float32)))
    return merged, top + jnp.log2(total)


def kernel(
    query_table, block_table, key_row, queries, keys, values, weight, projected,
    kv, qx, att, lse, early, early_lse, late, late_lse, own, w, out,
    local_sem, z_send, z_recv, core_send, core_recv, x_send, x_recv,
    early_send, early_recv, early_lse_send, early_lse_recv,
    late_send, late_recv, late_lse_send, late_lse_recv,
    y_send, y_recv, y2_send, y2_recv, out_sem,
):
    me, y = lax.axis_index("dp"), lax.axis_index("tensor")
    z, x, c = me // (NX * NC), (me // NC) % NX, me % NC

    def at(z, x, c):
        return ((z * NX + x) * NC + c, y)

    z_near = [at((z + 1) % NZ, x, c), at((z + NZ - 1) % NZ, x, c)]
    x_near = [at(z, (x + 1) % NX, c), at(z, (x + NX - 1) % NX, c)]
    y_near = [(me, (y + 1) % NY), (me, (y + NY - 1) % NY)]
    partner = at(z, x, 1 - c)

    def remote(src, dst, send, recv, device):
        return pltpu.make_async_remote_copy(
            src_ref=src, dst_ref=dst, send_sem=send, recv_sem=recv, device_id=device, device_id_type=MESH
        )

    loads = [
        pltpu.make_async_copy(keys, kv.at[0, 0, 0], local_sem.at[0]),
        pltpu.make_async_copy(values, kv.at[0, 0, 1], local_sem.at[1]),
        pltpu.make_async_copy(queries, qx.at[0], local_sem.at[2]),
    ]
    for load in loads:
        load.start()
    weight_load = pltpu.make_async_copy(weight, w, local_sem.at[3])
    weight_load.start()

    barrier = pltpu.get_barrier_semaphore()
    for device in z_near + x_near + y_near + [partner]:
        pl.semaphore_signal(barrier, inc=1, device_id=device, device_id_type=MESH)
    pl.semaphore_wait(barrier, 7)
    for load in loads:
        load.wait()

    started = []

    def start(copy):
        copy.start()
        started.append(copy)

    def z_copy(way, hop, t):
        src = (NZ - hop) % NZ if way == 0 else hop
        dst = NZ - hop - 1 if way == 0 else hop + 1
        return remote(
            kv.at[0, src, t], kv.at[0, dst, t], z_send.at[way, hop, t], z_recv.at[way, hop, t], z_near[way]
        )

    def z_goes(way, hop, t):
        return hop < 3 or (hop == 3 and t == way)

    def core_copy(d, t):
        return remote(kv.at[0, d, t], kv.at[1, d, t], core_send.at[d, t], core_recv.at[d, t], partner)

    def x_copy(way, n):
        g = n if n < 4 else n - 4 + 2 * way
        src, dst = (0, 3 - 2 * way) if n < 4 else (3 - 2 * way, 2)
        rows = pl.ds(g * GROUP, GROUP)
        return remote(qx.at[src, rows], qx.at[dst, rows], x_send.at[way, n], x_recv.at[way, n], x_near[way])

    for t in range(2):
        for way in range(2):
            start(z_copy(way, 0, t))
    for n in range(4):
        for way in range(2):
            start(x_copy(way, n))
    for t in range(2):
        start(core_copy(0, t))

    for hop in range(4):
        for t in range(2):
            for way in range(2):
                if not z_goes(way, hop, t):
                    continue
                z_copy(way, hop, t).wait_recv()
                if z_goes(way, hop + 1, t):
                    start(z_copy(way, hop + 1, t))
                start(core_copy(NZ - hop - 1 if way == 0 else hop + 1, t))
            n = 2 * hop + t
            if n < 4:
                for way in range(2):
                    x_copy(way, n).wait_recv()
                    if n // 2 == way:
                        start(x_copy(way, 4 + n % 2))
            elif n < 6:
                for way in range(2):
                    x_copy(way, n).wait_recv()
    for d in range(NZ):
        for t in range(2):
            core_copy(d, t).wait_recv()

    scale = LOG2E / HEAD_SIZE**0.5

    def attend_four(r, g, half):
        base = pl.multiple_of(g * GROUP + half * HALF, HALF)
        eye = diagonal()
        row_in_block = lax.broadcasted_iota(jnp.int32, (4 * ROWS, 1), 0) % ROWS
        sums = []
        for b in range(4):
            n = r * BLOCKS + g * 8 + half * 4 + b
            pack, place, begin = query_table[n], query_table[128 + n], query_table[256 + n]
            rows = pl.ds(base + b * ROWS, ROWS)
            q = heads_down(qx[r, rows, :])
            at_block = [block_table[pack * 16 + j] for j in range(16)]
            key_tile = jnp.concatenate([kv[j // NZ, j % NZ, 0, at_block[j]] for j in range(16)], axis=0)
            value_tile = jnp.concatenate([kv[j // NZ, j % NZ, 1, at_block[j]] for j in range(16)], axis=0)
            scores = lax.dot_general(
                q, key_tile, (((1,), (1,)), ((), ())), preferred_element_type=jnp.float32
            )
            key_at = key_row[pl.ds(pack, 1), :]
            key_at = jnp.where(key_at >= begin, key_at, FAR)
            scores = jnp.where(key_at <= place * ROWS + row_in_block, scores * scale, NEG)
            top = jnp.max(scores, axis=1, keepdims=True)
            terms = jnp.exp2(scores - top)
            total = jnp.sum(terms, axis=1, keepdims=True)
            mixed = jnp.dot(terms.astype(jnp.bfloat16), value_tile, preferred_element_type=jnp.float32)
            att[r, rows, :] = heads_across(mixed / total).astype(jnp.bfloat16)
            sums.append(jnp.sum(jnp.where(eye, top + jnp.log2(total), 0.0), axis=0, keepdims=True))
        lse[r, g, half] = jnp.concatenate(sums + [jnp.zeros((4, HEAD_SIZE), jnp.float32)], axis=0)

    def attend(g, first, last):
        def step(u, carry):
            v = u // 2
            attend_four((6 - v) % 4, g + (3 - v) // 3, u % 2)
            return carry

        lax.fori_loop(first, last, step, 0)

    def early_copies(g, way):
        rows = pl.ds(g * GROUP + way * HALF, HALF)
        return [
            remote(
                att.at[2, rows], early.at[way, g], early_send.at[way, g], early_recv.at[way, g], x_near[way]
            ),
            remote(
                lse.at[2, g, way], early_lse.at[way, g],
                early_lse_send.at[way, g], early_lse_recv.at[way, g], x_near[way],
            ),
        ]

    def late_copies(g, way, half):
        r = 1 + 2 * way
        rows = pl.ds(g * GROUP + half * HALF, HALF)
        return [
            remote(
                att.at[r, rows], late.at[way, rows],
                late_send.at[way, g, half], late_recv.at[way, g, half], x_near[way],
            ),
            remote(
                lse.at[r, g, half], late_lse.at[way, g, half],
                late_lse_send.at[way, g, half], late_lse_recv.at[way, g, half], x_near[way],
            ),
        ]

    def y_copy(g, way):
        rows = pl.ds(g * GROUP, GROUP)
        return remote(
            own.at[0, rows], own.at[3 - 2 * way, rows], y_send.at[way, g], y_recv.at[way, g], y_near[way]
        )

    def y2_copy(g, way):
        rows = pl.ds(g * GROUP + way * HALF, HALF)
        return remote(
            own.at[3 - 2 * way, rows], own.at[2, rows], y2_send.at[way, g], y2_recv.at[way, g], y_near[way]
        )

    def out_copy(g):
        rows = pl.ds(g * GROUP, GROUP)
        return pltpu.make_async_copy(out.at[rows], projected.at[rows], out_sem.at[g])

    def store_merged(ref_rows, merged):
        for b in range(4):
            ref_rows(b, merged[b].astype(jnp.bfloat16))

    def relay(g):
        for way in range(2):
            r = 1 + 2 * way
            for copy in early_copies(g, way):
                copy.wait_recv()
            first = g * GROUP + way * HALF
            merged, total = merge(
                [(att[r, first : first + HALF, :], lse[r, g, way]), (early[way, g], early_lse[way, g])]
            )
            for b in range(4):
                att[r, first + b * ROWS : first + (b + 1) * ROWS, :] = merged[b].astype(jnp.bfloat16)
            lse[r, g, way] = total
            for copy in late_copies(g, way, way):
                start(copy)

    def home(g):
        for way in range(2):
            for half in range(2):
                for copy in late_copies(g, way, half):
                    copy.wait_recv()
        row_in_block = lax.broadcasted_iota(jnp.int32, (ROWS, 1), 0)
        for half in range(2):
            first = g * GROUP + half * HALF
            rows = slice(first, first + HALF)
            merged, _ = merge(
                [(att[0, rows, :], lse[0, g, half])]
                + [(late[way, rows, :], late_lse[way, g, half]) for way in range(2)]
            )
            for b in range(4):
                left = query_table[384 + g * 8 + half * 4 + b]
                kept = jnp.where(row_in_block < left, merged[b], 0.0)
                own[0, first + b * ROWS : first + (b + 1) * ROWS, :] = kept.astype(jnp.bfloat16)
        for way in range(2):
            start(y_copy(g, way))

    def pass_on(g):
        for way in range(2):
            y_copy(g, way).wait_recv()
            start(y2_copy(g, way))

    def project(g):
        for way in range(2):
            y2_copy(g, way).wait_recv()
        rows = slice(g * GROUP, (g + 1) * GROUP)

        def columns(n, carry):
            cols = pl.ds(pl.multiple_of(n * 256, 256), 256)
            total = jnp.zeros((GROUP, 256), jnp.float32)
            for r in range(NY):
                depth = pl.ds(pl.multiple_of(((y + r) % NY) * COLS, COLS), COLS)
                total += jnp.dot(own[r, rows, :], w[depth, cols], preferred_element_type=jnp.float32)
            out[rows, cols] = total.astype(jnp.bfloat16)
            return carry

        lax.fori_loop(0, 4, columns, 0)
        out_copy(g).start()

    attend(-1, 0, 2)
    for way in range(2):
        for copy in early_copies(0, way):
            start(copy)
    weight_load.wait()
    for g in range(7):
        if g < 4:
            attend(g, 0 if g < 3 else 2, 8)
            for way in range(2):
                if g < 3:
                    for copy in early_copies(g + 1, way):
                        start(copy)
                for copy in late_copies(g, way, 1 - way):
                    start(copy)
            relay(g)
        if 1 <= g < 5:
            home(g - 1)
        if 2 <= g < 6:
            pass_on(g - 2)
        if 3 <= g:
            project(g - 3)
    for g in range(4):
        out_copy(g).wait()
    for copy in started:
        copy.wait_send()


def body(queries, keys, values, out_weight, dest_slot, pack_slot, seq_start, seq_len):
    total_rows = BLOCKS * ROWS
    tables = lookup_tables(dest_slot, pack_slot, seq_start, seq_len)
    anywhere = pl.BlockSpec(memory_space=pl.ANY)
    smem = pl.BlockSpec(memory_space=pltpu.SMEM)
    bf16, f32, dma = jnp.bfloat16, jnp.float32, pltpu.SemaphoreType.DMA
    projected = pl.pallas_call(
        kernel,
        out_shape=jax.ShapeDtypeStruct((total_rows, out_weight.shape[1]), bf16),
        in_specs=[smem, smem, pl.BlockSpec(memory_space=pltpu.VMEM)] + [anywhere] * 4,
        out_specs=anywhere,
        scratch_shapes=[
            pltpu.VMEM((2, NZ, 2, BLOCKS, ROWS, HEAD_SIZE), bf16),
            pltpu.VMEM((NX, total_rows, COLS), bf16),
            pltpu.VMEM((NX, total_rows, COLS), bf16),
            pltpu.VMEM((NX, 4, 2, 8, HEAD_SIZE), f32),
            pltpu.VMEM((2, 4, HALF, COLS), bf16),
            pltpu.VMEM((2, 4, 8, HEAD_SIZE), f32),
            pltpu.VMEM((2, total_rows, COLS), bf16),
            pltpu.VMEM((2, 4, 2, 8, HEAD_SIZE), f32),
            pltpu.VMEM((NY, total_rows, COLS), bf16),
            pltpu.VMEM(out_weight.shape, bf16),
            pltpu.VMEM((total_rows, out_weight.shape[1]), bf16),
            dma((4,)),
            dma((2, 4, 2)), dma((2, 4, 2)), dma((NZ, 2)), dma((NZ, 2)), dma((2, 6)), dma((2, 6)),
            dma((2, 4)), dma((2, 4)), dma((2, 4)), dma((2, 4)),
            dma((2, 4, 2)), dma((2, 4, 2)), dma((2, 4, 2)), dma((2, 4, 2)),
            dma((2, 4)), dma((2, 4)), dma((2, 4)), dma((2, 4)), dma((4,)),
        ],
        compiler_params=pltpu.CompilerParams(
            collective_id=0, has_side_effects=True, vmem_limit_bytes=60 * 2**20
        ),
    )(
        *tables,
        queries.reshape(total_rows, COLS),
        keys,
        values,
        out_weight,
    )
    return projected.reshape(BLOCKS, ROWS, out_weight.shape[1])


def solution(mesh):
    placed = (
        P("dp", None, "tensor"),
        P("dp", None, "tensor"),
        P("dp", None, "tensor"),
        P(None, "tensor"),
        P("dp"),
        P("dp", None),
        P("dp", None),
        P("dp", None),
    )
    return jax.shard_map(
        body, mesh=mesh, in_specs=placed, out_specs=P("dp", None, "tensor"), check_vma=False
    )
```

```python
import functools

import jax
import jax.numpy as jnp
from jax import lax
from jax.experimental import pallas as pl
from jax.experimental.pallas import tpu as pltpu
from jax.sharding import PartitionSpec as P

MESH = pl.DeviceIdType.MESH
HEAD_SIZE = 128
NZ, NX, NC, NY = 8, 4, 2, 4
BLOCKS, ROWS, COLS = 32, 32, 512
GROUP = 256
HALF = 128
NEG = -1e30
FAR = 1 << 20
LOG2E = 1.4426950408889634


N_PACKS = NZ * NX * NC
ARRIVAL = (0, 1, 7, 2, 6, 3, 5, 4)
PART = 256
PIECES = ((0, 6), (6, 14), (14, 22), (22, 24), (24, 32))


def heads_down(tile):
    return jnp.concatenate([tile[:, h * HEAD_SIZE : (h + 1) * HEAD_SIZE] for h in range(4)], axis=0)


def heads_across(tile):
    return jnp.concatenate([tile[h * ROWS : (h + 1) * ROWS] for h in range(4)], axis=1)


def diagonal():
    shape = (HEAD_SIZE, HEAD_SIZE)
    return lax.broadcasted_iota(jnp.int32, shape, 0) == lax.broadcasted_iota(jnp.int32, shape, 1)


def merge(parts):
    top = functools.reduce(jnp.maximum, [s for _, s in parts])
    shares = [jnp.exp2(s - top) for _, s in parts]
    total = functools.reduce(jnp.add, shares)
    shares = [s / total for s in shares]
    eye = diagonal()
    merged = []
    for b in range(4):
        weights = jnp.concatenate(
            [jnp.where(eye, s[b : b + 1], 0.0).astype(jnp.bfloat16) for s in shares], axis=1
        )
        outputs = jnp.concatenate([heads_down(o[b * ROWS : (b + 1) * ROWS]) for o, _ in parts], axis=0)
        merged.append(heads_across(jnp.dot(weights, outputs, preferred_element_type=jnp.float32)))
    return merged, top + jnp.log2(total)


def lookup_tables(table):
    me = lax.axis_index("dp")
    z, x, c = me // (NX * NC), (me // NC) % NX, me % NC
    count = jnp.arange(BLOCKS, dtype=jnp.int32)
    dest, sources = table[:, :32], table[:, 32:64]
    query_loader = (z * NX + (x + jnp.arange(NX)) % NX) * NC + c
    pack = jnp.take(dest, query_loader, axis=0).reshape(-1)
    rows = jnp.take(table, pack, axis=0)
    loader = jnp.repeat(query_loader, BLOCKS)[:, None]
    place = jnp.sum(jnp.where(rows[:, 32:64] == loader, count, 0), axis=1)
    starts = rows[:, 64:96]
    begin = jnp.max(jnp.where(starts <= place[:, None] * ROWS, starts, 0), axis=1)
    length = jnp.sum(jnp.where(starts == begin[:, None], rows[:, 96:], 0), axis=1)
    left = begin + length - place * ROWS
    key_z = jnp.repeat((z + jnp.array(ARRIVAL, jnp.int32)) % NZ, NC)
    key_c = jnp.tile((c + jnp.arange(NC)) % NC, NZ)
    key_loader = (key_z * NX + x) * NC + key_c
    found = sources[:, None, :] == key_loader[None, :, None]
    position = jnp.sum(jnp.where(found, count, 0), axis=2)
    position = jnp.where(jnp.any(found, axis=2), position * ROWS, FAR)
    key_row = (position[:, :, None] + jnp.arange(ROWS, dtype=jnp.int32)).reshape(N_PACKS, NC * NZ * ROWS)
    packs = jnp.arange(N_PACKS, dtype=jnp.int32)
    held = jnp.take(dest, key_loader, axis=0)[None] == packs[:, None, None]
    block = jnp.sum(jnp.where(held, count, 0), axis=2)
    query_table = jnp.concatenate([pack, place, begin, left[:BLOCKS]]).astype(jnp.int32)
    return query_table, block.reshape(-1).astype(jnp.int32), key_row.astype(jnp.int32)


def share_tables(mine, tab, own_sem, x_send, x_recv, z_send, z_recv):
    me, y = lax.axis_index("dp"), lax.axis_index("tensor")
    z, seat = me // 8, me % 8
    keep = pltpu.make_async_copy(mine, tab.at[pl.ds(me, 1)], own_sem)
    keep.start()
    plane = [(z * 8 + (seat + o) % 8, y) for o in range(1, 8)]
    column = [(((z + o) % NZ) * 8 + seat, y) for o in range(1, 8)]
    barrier = pltpu.get_barrier_semaphore()
    for device in plane + column:
        pl.semaphore_signal(barrier, inc=1, device_id=device, device_id_type=MESH)
    pl.semaphore_wait(barrier, 14)

    def in_plane(o, row):
        return pltpu.make_async_remote_copy(
            src_ref=mine, dst_ref=tab.at[pl.ds(row, 1)], send_sem=x_send.at[o], recv_sem=x_recv.at[o],
            device_id=plane[o], device_id_type=MESH,
        )

    def along_z(o, zz):
        rows = pl.ds(pl.multiple_of(zz * 8, 8), 8)
        return pltpu.make_async_remote_copy(
            src_ref=tab.at[rows], dst_ref=tab.at[rows], send_sem=z_send.at[o], recv_sem=z_recv.at[o],
            device_id=column[o], device_id_type=MESH,
        )

    for o in range(7):
        in_plane(o, me).start()
    keep.wait()
    for o in range(7):
        in_plane(o, z * 8 + (seat + 7 - o) % 8).wait_recv()
    for o in range(7):
        along_z(o, z).start()
    for o in range(7):
        along_z(o, (z + 7 - o) % NZ).wait_recv()
    for o in range(7):
        in_plane(o, me).wait_send()
        along_z(o, z).wait_send()


def kernel(query_table, block_table, key_row, queries, keys, values, weight, projected, *scratch):
    kv = [[scratch[(side * NZ + d) * 2 : (side * NZ + d) * 2 + 2] for d in range(NZ)] for side in range(2)]
    (
        packed, qx, first_att, first_lse, att, lse, early, early_lse, late, late_lse, own, w, out,
        local_sem, z_send, z_recv, core_send, core_recv, x_send, x_recv,
        early_send, early_recv, early_lse_send, early_lse_recv,
        late_send, late_recv, late_lse_send, late_lse_recv,
        y_send, y_recv, y2_send, y2_recv, out_sem,
    ) = scratch[32:]
    me, y = lax.axis_index("dp"), lax.axis_index("tensor")
    z, x, c = me // (NX * NC), (me // NC) % NX, me % NC

    def at(z, x, c):
        return ((z * NX + x) * NC + c, y)

    z_near = [at((z + 1) % NZ, x, c), at((z + NZ - 1) % NZ, x, c)]
    x_near = [at(z, (x + 1) % NX, c), at(z, (x + NX - 1) % NX, c)]
    y_near = [(me, (y + 1) % NY), (me, (y + NY - 1) % NY)]
    partner = at(z, x, 1 - c)

    def remote(src, dst, send, recv, device):
        return pltpu.make_async_remote_copy(
            src_ref=src, dst_ref=dst, send_sem=send, recv_sem=recv, device_id=device, device_id_type=MESH
        )

    loads = [
        pltpu.make_async_copy(keys, kv[0][0][0], local_sem.at[0]),
        pltpu.make_async_copy(values, kv[0][0][1], local_sem.at[1]),
        pltpu.make_async_copy(queries, qx.at[0], local_sem.at[2]),
    ]
    for load in loads:
        load.start()
    weight_load = pltpu.make_async_copy(weight, w, local_sem.at[3])
    weight_load.start()

    barrier = pltpu.get_barrier_semaphore()
    for device in z_near + x_near + y_near + [partner]:
        pl.semaphore_signal(barrier, inc=1, device_id=device, device_id_type=MESH)
    pl.semaphore_wait(barrier, 7)
    for load in loads:
        load.wait()

    started = []

    def start(copy):
        copy.start()
        started.append(copy)

    def z_copy(way, hop, t):
        src = (NZ - hop) % NZ if way == 0 else hop
        dst = NZ - hop - 1 if way == 0 else hop + 1
        return remote(
            kv[0][src][t], kv[0][dst][t], z_send.at[way, hop, t], z_recv.at[way, hop, t], z_near[way]
        )

    def z_goes(way, hop, t):
        return hop < 3 or (hop == 3 and t == way)

    def core_copy(d, t):
        return remote(kv[0][d][t], kv[1][d][t], core_send.at[d, t], core_recv.at[d, t], partner)

    def x_copy(way, n):
        g = n if n < 4 else n - 4 + 2 * way
        src, dst = (0, 3 - 2 * way) if n < 4 else (3 - 2 * way, 2)
        rows = pl.ds(g * GROUP, GROUP)
        return remote(qx.at[src, rows], qx.at[dst, rows], x_send.at[way, n], x_recv.at[way, n], x_near[way])

    def pack(side, d, t):
        j = ARRIVAL.index(d) * 2 + side

        def step(n, carry):
            for p in range(8):
                packed[n * 8 + p, t, j * ROWS : (j + 1) * ROWS, :] = kv[side][d][t][block_table[(n * 8 + p) * 16 + j]]
            return carry

        lax.fori_loop(0, N_PACKS // 8, step, 0)

    scale = LOG2E / HEAD_SIZE**0.5

    def attend_four(r, g, half, part):
        base = pl.multiple_of(g * GROUP + half * HALF, HALF)
        eye = diagonal()
        row_in_block = lax.broadcasted_iota(jnp.int32, (4 * ROWS, 1), 0) % ROWS
        keys_of_part = slice(part * PART, (part + 1) * PART)
        outputs, sums = [], []
        for b in range(4):
            n = r * BLOCKS + g * 8 + half * 4 + b
            to, place, begin = query_table[n], query_table[128 + n], query_table[256 + n]
            rows = pl.ds(base + b * ROWS, ROWS)
            q = heads_down(qx[r, rows, :])
            scores = lax.dot_general(
                q, packed[to, 0, keys_of_part, :], (((1,), (1,)), ((), ())), preferred_element_type=jnp.float32
            )
            key_at = key_row[pl.ds(to, 1), keys_of_part]
            key_at = jnp.where(key_at >= begin, key_at, FAR)
            scores = jnp.where(key_at <= place * ROWS + row_in_block, scores * scale, NEG)
            top = jnp.max(scores, axis=1, keepdims=True)
            terms = jnp.exp2(scores - top)
            total = jnp.sum(terms, axis=1, keepdims=True)
            mixed = jnp.dot(terms.astype(jnp.bfloat16), packed[to, 1, keys_of_part, :], preferred_element_type=jnp.float32)
            outputs.append(heads_across(mixed / total).astype(jnp.bfloat16))
            sums.append(jnp.sum(jnp.where(eye, top + jnp.log2(total), 0.0), axis=0, keepdims=True))
        sums = jnp.concatenate(sums + [jnp.zeros((4, HEAD_SIZE), jnp.float32)], axis=0)
        if part == 0:
            for b in range(4):
                first_att[r, pl.ds(base + b * ROWS, ROWS), :] = outputs[b]
            first_lse[r, g, half] = sums
            return
        merged, sums = merge(
            [
                (first_att[r, pl.ds(base, HALF), :], first_lse[r, g, half]),
                (jnp.concatenate(outputs, axis=0), sums),
            ]
        )
        for b in range(4):
            att[r, pl.ds(base + b * ROWS, ROWS), :] = merged[b].astype(jnp.bfloat16)
        lse[r, g, half] = sums

    def attend_first(first, last):
        def step(u, carry):
            v = u // 8
            attend_four(v + v // 2 - 2 * (v // 3), (u % 8) // 2, u % 2, 0)
            return carry

        lax.fori_loop(first, last, step, 0)

    def pack_all(blocks):
        for side, d, t in blocks:
            if side == 1:
                core_copy(d, t).wait_recv()
            pack(side, d, t)

    for way in range(2):
        start(z_copy(way, 0, 0))
    for n in range(4):
        for way in range(2):
            start(x_copy(way, n))
    for t in range(2):
        start(core_copy(0, t))
    for way in range(2):
        start(z_copy(way, 0, 1))
    pack_all([(0, 0, 0), (0, 0, 1), (1, 0, 0), (1, 0, 1)])

    arrived = []
    for hop in range(4):
        for t in range(2):
            due, arrived = arrived, []
            for way in range(2):
                if not z_goes(way, hop, t):
                    continue
                z_copy(way, hop, t).wait_recv()
                if z_goes(way, hop + 1, t):
                    start(z_copy(way, hop + 1, t))
                d = NZ - hop - 1 if way == 0 else hop + 1
                start(core_copy(d, t))
                arrived += [(0, d, t), (1, d, t)]
            n = 2 * hop + t
            if n < 4:
                for way in range(2):
                    x_copy(way, n).wait_recv()
                    if n // 2 == way:
                        start(x_copy(way, 4 + n % 2))
            elif n < 6:
                for way in range(2):
                    x_copy(way, n).wait_recv()
            if n == 3:
                due, arrived = due + sorted(arrived), []
            pack_all(due)
            if n >= 3:
                attend_first(*PIECES[n - 3])
    pack_all(sorted(arrived))

    def attend(g, first, last):
        def step(u, carry):
            v = u // 2
            attend_four((6 - v) % 4, g + (3 - v) // 3, u % 2, 1)
            return carry

        lax.fori_loop(first, last, step, 0)

    def early_copies(g, way):
        rows = pl.ds(g * GROUP + way * HALF, HALF)
        return [
            remote(
                att.at[2, rows], early.at[way, g], early_send.at[way, g], early_recv.at[way, g], x_near[way]
            ),
            remote(
                lse.at[2, g, way], early_lse.at[way, g],
                early_lse_send.at[way, g], early_lse_recv.at[way, g], x_near[way],
            ),
        ]

    def late_copies(g, way, half):
        r = 1 + 2 * way
        rows = pl.ds(g * GROUP + half * HALF, HALF)
        return [
            remote(
                att.at[r, rows], late.at[way, rows],
                late_send.at[way, g, half], late_recv.at[way, g, half], x_near[way],
            ),
            remote(
                lse.at[r, g, half], late_lse.at[way, g, half],
                late_lse_send.at[way, g, half], late_lse_recv.at[way, g, half], x_near[way],
            ),
        ]

    def y_copy(g, way):
        rows = pl.ds(g * GROUP, GROUP)
        return remote(
            own.at[0, rows], own.at[3 - 2 * way, rows], y_send.at[way, g], y_recv.at[way, g], y_near[way]
        )

    def y2_copy(g, way):
        rows = pl.ds(g * GROUP + way * HALF, HALF)
        return remote(
            own.at[3 - 2 * way, rows], own.at[2, rows], y2_send.at[way, g], y2_recv.at[way, g], y_near[way]
        )

    def out_copy(g):
        rows = pl.ds(g * GROUP, GROUP)
        return pltpu.make_async_copy(out.at[rows], projected.at[rows], out_sem.at[g])

    def store_merged(ref_rows, merged):
        for b in range(4):
            ref_rows(b, merged[b].astype(jnp.bfloat16))

    def relay(g):
        for way in range(2):
            r = 1 + 2 * way
            for copy in early_copies(g, way):
                copy.wait_recv()
            first = g * GROUP + way * HALF
            merged, total = merge(
                [(att[r, first : first + HALF, :], lse[r, g, way]), (early[way, g], early_lse[way, g])]
            )
            for b in range(4):
                att[r, first + b * ROWS : first + (b + 1) * ROWS, :] = merged[b].astype(jnp.bfloat16)
            lse[r, g, way] = total
            for copy in late_copies(g, way, way):
                start(copy)

    def home(g):
        for way in range(2):
            for half in range(2):
                for copy in late_copies(g, way, half):
                    copy.wait_recv()
        row_in_block = lax.broadcasted_iota(jnp.int32, (ROWS, 1), 0)
        for half in range(2):
            first = g * GROUP + half * HALF
            rows = slice(first, first + HALF)
            merged, _ = merge(
                [(att[0, rows, :], lse[0, g, half])]
                + [(late[way, rows, :], late_lse[way, g, half]) for way in range(2)]
            )
            for b in range(4):
                left = query_table[384 + g * 8 + half * 4 + b]
                kept = jnp.where(row_in_block < left, merged[b], 0.0)
                own[0, first + b * ROWS : first + (b + 1) * ROWS, :] = kept.astype(jnp.bfloat16)
        for way in range(2):
            start(y_copy(g, way))

    def pass_on(g):
        for way in range(2):
            y_copy(g, way).wait_recv()
            start(y2_copy(g, way))

    def project(g):
        for way in range(2):
            y2_copy(g, way).wait_recv()
        rows = slice(g * GROUP, (g + 1) * GROUP)

        def columns(n, carry):
            cols = pl.ds(pl.multiple_of(n * 256, 256), 256)
            total = jnp.zeros((GROUP, 256), jnp.float32)
            for r in range(NY):
                depth = pl.ds(pl.multiple_of(((y + r) % NY) * COLS, COLS), COLS)
                total += jnp.dot(own[r, rows, :], w[depth, cols], preferred_element_type=jnp.float32)
            out[rows, cols] = total.astype(jnp.bfloat16)
            return carry

        lax.fori_loop(0, 4, columns, 0)
        out_copy(g).start()

    attend(-1, 0, 2)
    for way in range(2):
        for copy in early_copies(0, way):
            start(copy)
    weight_load.wait()
    for g in range(7):
        if g < 4:
            attend(g, 0 if g < 3 else 2, 8)
            for way in range(2):
                if g < 3:
                    for copy in early_copies(g + 1, way):
                        start(copy)
                for copy in late_copies(g, way, 1 - way):
                    start(copy)
            relay(g)
        if 1 <= g < 5:
            home(g - 1)
        if 2 <= g < 6:
            pass_on(g - 2)
        if 3 <= g:
            project(g - 3)
    for g in range(4):
        out_copy(g).wait()
    for copy in started:
        copy.wait_send()


def body(queries, keys, values, out_weight, dest_slot, pack_slot, seq_start, seq_len):
    total_rows = BLOCKS * ROWS
    mine = jnp.concatenate([dest_slot, pack_slot[0], seq_start[0], seq_len[0]])[None]
    anywhere = pl.BlockSpec(memory_space=pl.ANY)
    smem = pl.BlockSpec(memory_space=pltpu.SMEM)
    bf16, f32, dma = jnp.bfloat16, jnp.float32, pltpu.SemaphoreType.DMA
    table = pl.pallas_call(
        share_tables,
        out_shape=jax.ShapeDtypeStruct((N_PACKS, 128), jnp.int32),
        in_specs=[pl.BlockSpec(memory_space=pltpu.VMEM)],
        out_specs=pl.BlockSpec(memory_space=pltpu.VMEM),
        scratch_shapes=[dma(())] + [dma((7,))] * 4,
        compiler_params=pltpu.CompilerParams(collective_id=1, has_side_effects=True),
    )(mine)
    projected = pl.pallas_call(
        kernel,
        out_shape=jax.ShapeDtypeStruct((total_rows, out_weight.shape[1]), bf16),
        in_specs=[smem, smem, pl.BlockSpec(memory_space=pltpu.VMEM)] + [anywhere] * 4,
        out_specs=anywhere,
        scratch_shapes=[
            *[pltpu.VMEM((BLOCKS, ROWS, HEAD_SIZE), bf16)] * 32,
            pltpu.VMEM((N_PACKS, 2, 16 * ROWS, HEAD_SIZE), bf16),
            pltpu.VMEM((NX, total_rows, COLS), bf16),
            pltpu.VMEM((NX, total_rows, COLS), bf16),
            pltpu.VMEM((NX, 4, 2, 8, HEAD_SIZE), f32),
            pltpu.VMEM((NX, total_rows, COLS), bf16),
            pltpu.VMEM((NX, 4, 2, 8, HEAD_SIZE), f32),
            pltpu.VMEM((2, 4, HALF, COLS), bf16),
            pltpu.VMEM((2, 4, 8, HEAD_SIZE), f32),
            pltpu.VMEM((2, total_rows, COLS), bf16),
            pltpu.VMEM((2, 4, 2, 8, HEAD_SIZE), f32),
            pltpu.VMEM((NY, total_rows, COLS), bf16),
            pltpu.VMEM(out_weight.shape, bf16),
            pltpu.VMEM((total_rows, out_weight.shape[1]), bf16),
            dma((4,)),
            dma((2, 4, 2)), dma((2, 4, 2)), dma((NZ, 2)), dma((NZ, 2)), dma((2, 6)), dma((2, 6)),
            dma((2, 4)), dma((2, 4)), dma((2, 4)), dma((2, 4)),
            dma((2, 4, 2)), dma((2, 4, 2)), dma((2, 4, 2)), dma((2, 4, 2)),
            dma((2, 4)), dma((2, 4)), dma((2, 4)), dma((2, 4)), dma((4,)),
        ],
        compiler_params=pltpu.CompilerParams(
            collective_id=0, has_side_effects=True, vmem_limit_bytes=60 * 2**20
        ),
    )(
        *lookup_tables(table),
        queries.reshape(total_rows, COLS),
        keys,
        values,
        out_weight,
    )
    return projected.reshape(BLOCKS, ROWS, out_weight.shape[1])


def solution(mesh):
    placed = (
        P("dp", None, "tensor"),
        P("dp", None, "tensor"),
        P("dp", None, "tensor"),
        P(None, "tensor"),
        P("dp"),
        P("dp", None),
        P("dp", None),
        P("dp", None),
    )
    return jax.shard_map(
        body, mesh=mesh, in_specs=placed, out_specs=P("dp", None, "tensor"), check_vma=False
    )
```

```python
import functools

import jax
import jax.numpy as jnp
from jax import lax
from jax.experimental import pallas as pl
from jax.experimental.pallas import tpu as pltpu
from jax.sharding import PartitionSpec as P

MESH = pl.DeviceIdType.MESH
HEAD_SIZE = 128
NZ, NX, NC, NY = 8, 4, 2, 4
BLOCKS, ROWS, COLS = 32, 32, 512
GROUP = 256
HALF = 128
NEG = -1e30
FAR = 1 << 20
LOG2E = 1.4426950408889634


N_PACKS = NZ * NX * NC
ARRIVAL = (0, 1, 7, 2, 6, 3, 5, 4)


def heads_down(tile):
    return jnp.concatenate([tile[:, h * HEAD_SIZE : (h + 1) * HEAD_SIZE] for h in range(4)], axis=0)


def heads_across(tile):
    return jnp.concatenate([tile[h * ROWS : (h + 1) * ROWS] for h in range(4)], axis=1)


def diagonal():
    shape = (HEAD_SIZE, HEAD_SIZE)
    return lax.broadcasted_iota(jnp.int32, shape, 0) == lax.broadcasted_iota(jnp.int32, shape, 1)


def merge(parts):
    top = functools.reduce(jnp.maximum, [s for _, s in parts])
    shares = [jnp.exp2(s - top) for _, s in parts]
    total = functools.reduce(jnp.add, shares)
    shares = [s / total for s in shares]
    eye = diagonal()
    merged = []
    for b in range(4):
        weights = jnp.concatenate(
            [jnp.where(eye, s[b : b + 1], 0.0).astype(jnp.bfloat16) for s in shares], axis=1
        )
        outputs = jnp.concatenate([heads_down(o[b * ROWS : (b + 1) * ROWS]) for o, _ in parts], axis=0)
        merged.append(heads_across(jnp.dot(weights, outputs, preferred_element_type=jnp.float32)))
    return merged, top + jnp.log2(total)


def lookup_tables(table):
    me = lax.axis_index("dp")
    z, x, c = me // (NX * NC), (me // NC) % NX, me % NC
    count = jnp.arange(BLOCKS, dtype=jnp.int32)
    dest, sources = table[:, :32], table[:, 32:64]
    query_loader = (z * NX + (x + jnp.arange(NX)) % NX) * NC + c
    pack = jnp.take(dest, query_loader, axis=0).reshape(-1)
    rows = jnp.take(table, pack, axis=0)
    loader = jnp.repeat(query_loader, BLOCKS)[:, None]
    place = jnp.sum(jnp.where(rows[:, 32:64] == loader, count, 0), axis=1)
    starts = rows[:, 64:96]
    begin = jnp.max(jnp.where(starts <= place[:, None] * ROWS, starts, 0), axis=1)
    length = jnp.sum(jnp.where(starts == begin[:, None], rows[:, 96:], 0), axis=1)
    left = begin + length - place * ROWS
    key_z = jnp.repeat((z + jnp.array(ARRIVAL, jnp.int32)) % NZ, NC)
    key_c = jnp.tile((c + jnp.arange(NC)) % NC, NZ)
    key_loader = (key_z * NX + x) * NC + key_c
    found = sources[:, None, :] == key_loader[None, :, None]
    position = jnp.sum(jnp.where(found, count, 0), axis=2)
    position = jnp.where(jnp.any(found, axis=2), position * ROWS, FAR)
    key_row = (position[:, :, None] + jnp.arange(ROWS, dtype=jnp.int32)).reshape(N_PACKS, NC * NZ * ROWS)
    packs = jnp.arange(N_PACKS, dtype=jnp.int32)
    held = jnp.take(dest, key_loader, axis=0)[None] == packs[:, None, None]
    block = jnp.sum(jnp.where(held, count, 0), axis=2)
    query_table = jnp.concatenate([pack, place, begin, left[:BLOCKS]]).astype(jnp.int32)
    return query_table, block.reshape(-1).astype(jnp.int32), key_row.astype(jnp.int32)


def share_tables(mine, tab, own_sem, x_send, x_recv, z_send, z_recv):
    me, y = lax.axis_index("dp"), lax.axis_index("tensor")
    z, seat = me // 8, me % 8
    keep = pltpu.make_async_copy(mine, tab.at[pl.ds(me, 1)], own_sem)
    keep.start()
    plane = [(z * 8 + (seat + o) % 8, y) for o in range(1, 8)]
    column = [(((z + o) % NZ) * 8 + seat, y) for o in range(1, 8)]
    barrier = pltpu.get_barrier_semaphore()
    for device in plane + column:
        pl.semaphore_signal(barrier, inc=1, device_id=device, device_id_type=MESH)
    pl.semaphore_wait(barrier, 14)

    def in_plane(o, row):
        return pltpu.make_async_remote_copy(
            src_ref=mine, dst_ref=tab.at[pl.ds(row, 1)], send_sem=x_send.at[o], recv_sem=x_recv.at[o],
            device_id=plane[o], device_id_type=MESH,
        )

    def along_z(o, zz):
        rows = pl.ds(pl.multiple_of(zz * 8, 8), 8)
        return pltpu.make_async_remote_copy(
            src_ref=tab.at[rows], dst_ref=tab.at[rows], send_sem=z_send.at[o], recv_sem=z_recv.at[o],
            device_id=column[o], device_id_type=MESH,
        )

    for o in range(7):
        in_plane(o, me).start()
    keep.wait()
    for o in range(7):
        in_plane(o, z * 8 + (seat + 7 - o) % 8).wait_recv()
    for o in range(7):
        along_z(o, z).start()
    for o in range(7):
        along_z(o, (z + 7 - o) % NZ).wait_recv()
    for o in range(7):
        in_plane(o, me).wait_send()
        along_z(o, z).wait_send()


def kernel(query_table, block_table, key_row, queries, keys, values, weight, projected, *scratch):
    kv = [[scratch[(side * NZ + d) * 2 : (side * NZ + d) * 2 + 2] for d in range(NZ)] for side in range(2)]
    (
        packed, qx, att, lse, early, early_lse, late, late_lse, own, w, out,
        local_sem, z_send, z_recv, core_send, core_recv, x_send, x_recv,
        early_send, early_recv, early_lse_send, early_lse_recv,
        late_send, late_recv, late_lse_send, late_lse_recv,
        y_send, y_recv, y2_send, y2_recv, out_sem,
    ) = scratch[32:]
    me, y = lax.axis_index("dp"), lax.axis_index("tensor")
    z, x, c = me // (NX * NC), (me // NC) % NX, me % NC

    def at(z, x, c):
        return ((z * NX + x) * NC + c, y)

    z_near = [at((z + 1) % NZ, x, c), at((z + NZ - 1) % NZ, x, c)]
    x_near = [at(z, (x + 1) % NX, c), at(z, (x + NX - 1) % NX, c)]
    y_near = [(me, (y + 1) % NY), (me, (y + NY - 1) % NY)]
    partner = at(z, x, 1 - c)

    def remote(src, dst, send, recv, device):
        return pltpu.make_async_remote_copy(
            src_ref=src, dst_ref=dst, send_sem=send, recv_sem=recv, device_id=device, device_id_type=MESH
        )

    loads = [
        pltpu.make_async_copy(keys, kv[0][0][0], local_sem.at[0]),
        pltpu.make_async_copy(values, kv[0][0][1], local_sem.at[1]),
        pltpu.make_async_copy(queries, qx.at[0], local_sem.at[2]),
    ]
    for load in loads:
        load.start()
    weight_load = pltpu.make_async_copy(weight, w, local_sem.at[3])
    weight_load.start()

    barrier = pltpu.get_barrier_semaphore()
    for device in z_near + x_near + y_near + [partner]:
        pl.semaphore_signal(barrier, inc=1, device_id=device, device_id_type=MESH)
    pl.semaphore_wait(barrier, 7)
    for load in loads:
        load.wait()

    started = []

    def start(copy):
        copy.start()
        started.append(copy)

    def z_copy(way, hop, t):
        src = (NZ - hop) % NZ if way == 0 else hop
        dst = NZ - hop - 1 if way == 0 else hop + 1
        return remote(
            kv[0][src][t], kv[0][dst][t], z_send.at[way, hop, t], z_recv.at[way, hop, t], z_near[way]
        )

    def z_goes(way, hop, t):
        return hop < 3 or (hop == 3 and t == way)

    def core_copy(d, t):
        return remote(kv[0][d][t], kv[1][d][t], core_send.at[d, t], core_recv.at[d, t], partner)

    def x_copy(way, n):
        g = n if n < 4 else n - 4 + 2 * way
        src, dst = (0, 3 - 2 * way) if n < 4 else (3 - 2 * way, 2)
        rows = pl.ds(g * GROUP, GROUP)
        return remote(qx.at[src, rows], qx.at[dst, rows], x_send.at[way, n], x_recv.at[way, n], x_near[way])

    def pack(side, d, t):
        j = ARRIVAL.index(d) * 2 + side

        def step(n, carry):
            for p in range(8):
                packed[n * 8 + p, t, j * ROWS : (j + 1) * ROWS, :] = kv[side][d][t][block_table[(n * 8 + p) * 16 + j]]
            return carry

        lax.fori_loop(0, N_PACKS // 8, step, 0)

    scale = LOG2E / HEAD_SIZE**0.5

    def attend_four(r, g, half):
        base = pl.multiple_of(g * GROUP + half * HALF, HALF)
        eye = diagonal()
        row_in_block = lax.broadcasted_iota(jnp.int32, (4 * ROWS, 1), 0) % ROWS
        outputs, sums = [], []
        for b in range(4):
            n = r * BLOCKS + g * 8 + half * 4 + b
            to, place, begin = query_table[n], query_table[128 + n], query_table[256 + n]
            rows = pl.ds(base + b * ROWS, ROWS)
            q = heads_down(qx[r, rows, :])
            scores = lax.dot_general(
                q, packed[to, 0], (((1,), (1,)), ((), ())), preferred_element_type=jnp.float32
            )
            key_at = key_row[pl.ds(to, 1), :]
            key_at = jnp.where(key_at >= begin, key_at, FAR)
            scores = jnp.where(key_at <= place * ROWS + row_in_block, scores * scale, NEG)
            top = jnp.max(scores, axis=1, keepdims=True)
            terms = jnp.exp2(scores - top)
            total = jnp.sum(terms, axis=1, keepdims=True)
            mixed = jnp.dot(terms.astype(jnp.bfloat16), packed[to, 1], preferred_element_type=jnp.float32)
            outputs.append(heads_across(mixed / total).astype(jnp.bfloat16))
            sums.append(jnp.sum(jnp.where(eye, top + jnp.log2(total), 0.0), axis=0, keepdims=True))
        sums = jnp.concatenate(sums + [jnp.zeros((4, HEAD_SIZE), jnp.float32)], axis=0)
        for b in range(4):
            att[r, pl.ds(base + b * ROWS, ROWS), :] = outputs[b]
        lse[r, g, half] = sums

    def pack_all(blocks):
        for side, d, t in blocks:
            if side == 1:
                core_copy(d, t).wait_recv()
            pack(side, d, t)

    for way in range(2):
        start(z_copy(way, 0, 0))
    for n in range(4):
        for way in range(2):
            start(x_copy(way, n))
    for t in range(2):
        start(core_copy(0, t))
    for way in range(2):
        start(z_copy(way, 0, 1))
    pack_all([(0, 0, 0), (0, 0, 1), (1, 0, 0), (1, 0, 1)])

    arrived = []
    for hop in range(4):
        for t in range(2):
            due, arrived = arrived, []
            for way in range(2):
                if not z_goes(way, hop, t):
                    continue
                z_copy(way, hop, t).wait_recv()
                if z_goes(way, hop + 1, t):
                    start(z_copy(way, hop + 1, t))
                d = NZ - hop - 1 if way == 0 else hop + 1
                start(core_copy(d, t))
                arrived += [(0, d, t), (1, d, t)]
            n = 2 * hop + t
            if n < 4:
                for way in range(2):
                    x_copy(way, n).wait_recv()
                    if n // 2 == way:
                        start(x_copy(way, 4 + n % 2))
            elif n < 6:
                for way in range(2):
                    x_copy(way, n).wait_recv()
            pack_all(due)
    pack_all(sorted(arrived))

    def attend(g, first, last):
        def step(u, carry):
            v = u // 2
            attend_four((6 - v) % 4, g + (3 - v) // 3, u % 2)
            return carry

        lax.fori_loop(first, last, step, 0)

    def early_copies(g, way):
        rows = pl.ds(g * GROUP + way * HALF, HALF)
        return [
            remote(
                att.at[2, rows], early.at[way, g], early_send.at[way, g], early_recv.at[way, g], x_near[way]
            ),
            remote(
                lse.at[2, g, way], early_lse.at[way, g],
                early_lse_send.at[way, g], early_lse_recv.at[way, g], x_near[way],
            ),
        ]

    def late_copies(g, way, half):
        r = 1 + 2 * way
        rows = pl.ds(g * GROUP + half * HALF, HALF)
        return [
            remote(
                att.at[r, rows], late.at[way, rows],
                late_send.at[way, g, half], late_recv.at[way, g, half], x_near[way],
            ),
            remote(
                lse.at[r, g, half], late_lse.at[way, g, half],
                late_lse_send.at[way, g, half], late_lse_recv.at[way, g, half], x_near[way],
            ),
        ]

    def y_copy(g, way):
        rows = pl.ds(g * GROUP, GROUP)
        return remote(
            own.at[0, rows], own.at[3 - 2 * way, rows], y_send.at[way, g], y_recv.at[way, g], y_near[way]
        )

    def y2_copy(g, way):
        rows = pl.ds(g * GROUP + way * HALF, HALF)
        return remote(
            own.at[3 - 2 * way, rows], own.at[2, rows], y2_send.at[way, g], y2_recv.at[way, g], y_near[way]
        )

    def out_copy(g):
        rows = pl.ds(g * GROUP, GROUP)
        return pltpu.make_async_copy(out.at[rows], projected.at[rows], out_sem.at[g])

    def store_merged(ref_rows, merged):
        for b in range(4):
            ref_rows(b, merged[b].astype(jnp.bfloat16))

    def relay(g):
        for way in range(2):
            r = 1 + 2 * way
            for copy in early_copies(g, way):
                copy.wait_recv()
            first = g * GROUP + way * HALF
            merged, total = merge(
                [(att[r, first : first + HALF, :], lse[r, g, way]), (early[way, g], early_lse[way, g])]
            )
            for b in range(4):
                att[r, first + b * ROWS : first + (b + 1) * ROWS, :] = merged[b].astype(jnp.bfloat16)
            lse[r, g, way] = total
            for copy in late_copies(g, way, way):
                start(copy)

    def home(g):
        for way in range(2):
            for half in range(2):
                for copy in late_copies(g, way, half):
                    copy.wait_recv()
        row_in_block = lax.broadcasted_iota(jnp.int32, (ROWS, 1), 0)
        for half in range(2):
            first = g * GROUP + half * HALF
            rows = slice(first, first + HALF)
            merged, _ = merge(
                [(att[0, rows, :], lse[0, g, half])]
                + [(late[way, rows, :], late_lse[way, g, half]) for way in range(2)]
            )
            for b in range(4):
                left = query_table[384 + g * 8 + half * 4 + b]
                kept = jnp.where(row_in_block < left, merged[b], 0.0)
                own[0, first + b * ROWS : first + (b + 1) * ROWS, :] = kept.astype(jnp.bfloat16)
        for way in range(2):
            start(y_copy(g, way))

    def pass_on(g):
        for way in range(2):
            y_copy(g, way).wait_recv()
            start(y2_copy(g, way))

    def project(g):
        for way in range(2):
            y2_copy(g, way).wait_recv()
        rows = slice(g * GROUP, (g + 1) * GROUP)

        def columns(n, carry):
            cols = pl.ds(pl.multiple_of(n * 256, 256), 256)
            total = jnp.zeros((GROUP, 256), jnp.float32)
            for r in range(NY):
                depth = pl.ds(pl.multiple_of(((y + r) % NY) * COLS, COLS), COLS)
                total += jnp.dot(own[r, rows, :], w[depth, cols], preferred_element_type=jnp.float32)
            out[rows, cols] = total.astype(jnp.bfloat16)
            return carry

        lax.fori_loop(0, 4, columns, 0)
        out_copy(g).start()

    attend(-1, 0, 2)
    for way in range(2):
        for copy in early_copies(0, way):
            start(copy)
    weight_load.wait()
    for g in range(7):
        if g < 4:
            attend(g, 0 if g < 3 else 2, 8)
            for way in range(2):
                if g < 3:
                    for copy in early_copies(g + 1, way):
                        start(copy)
                for copy in late_copies(g, way, 1 - way):
                    start(copy)
            relay(g)
        if 1 <= g < 5:
            home(g - 1)
        if 2 <= g < 6:
            pass_on(g - 2)
        if 3 <= g:
            project(g - 3)
    for g in range(4):
        out_copy(g).wait()
    for copy in started:
        copy.wait_send()


def body(queries, keys, values, out_weight, dest_slot, pack_slot, seq_start, seq_len):
    total_rows = BLOCKS * ROWS
    mine = jnp.concatenate([dest_slot, pack_slot[0], seq_start[0], seq_len[0]])[None]
    anywhere = pl.BlockSpec(memory_space=pl.ANY)
    smem = pl.BlockSpec(memory_space=pltpu.SMEM)
    bf16, f32, dma = jnp.bfloat16, jnp.float32, pltpu.SemaphoreType.DMA
    table = pl.pallas_call(
        share_tables,
        out_shape=jax.ShapeDtypeStruct((N_PACKS, 128), jnp.int32),
        in_specs=[pl.BlockSpec(memory_space=pltpu.VMEM)],
        out_specs=pl.BlockSpec(memory_space=pltpu.VMEM),
        scratch_shapes=[dma(())] + [dma((7,))] * 4,
        compiler_params=pltpu.CompilerParams(collective_id=1, has_side_effects=True),
    )(mine)
    projected = pl.pallas_call(
        kernel,
        out_shape=jax.ShapeDtypeStruct((total_rows, out_weight.shape[1]), bf16),
        in_specs=[smem, smem, pl.BlockSpec(memory_space=pltpu.VMEM)] + [anywhere] * 4,
        out_specs=anywhere,
        scratch_shapes=[
            *[pltpu.VMEM((BLOCKS, ROWS, HEAD_SIZE), bf16)] * 32,
            pltpu.VMEM((N_PACKS, 2, 16 * ROWS, HEAD_SIZE), bf16),
            pltpu.VMEM((NX, total_rows, COLS), bf16),
            pltpu.VMEM((NX, total_rows, COLS), bf16),
            pltpu.VMEM((NX, 4, 2, 8, HEAD_SIZE), f32),
            pltpu.VMEM((2, 4, HALF, COLS), bf16),
            pltpu.VMEM((2, 4, 8, HEAD_SIZE), f32),
            pltpu.VMEM((2, total_rows, COLS), bf16),
            pltpu.VMEM((2, 4, 2, 8, HEAD_SIZE), f32),
            pltpu.VMEM((NY, total_rows, COLS), bf16),
            pltpu.VMEM(out_weight.shape, bf16),
            pltpu.VMEM((total_rows, out_weight.shape[1]), bf16),
            dma((4,)),
            dma((2, 4, 2)), dma((2, 4, 2)), dma((NZ, 2)), dma((NZ, 2)), dma((2, 6)), dma((2, 6)),
            dma((2, 4)), dma((2, 4)), dma((2, 4)), dma((2, 4)),
            dma((2, 4, 2)), dma((2, 4, 2)), dma((2, 4, 2)), dma((2, 4, 2)),
            dma((2, 4)), dma((2, 4)), dma((2, 4)), dma((2, 4)), dma((4,)),
        ],
        compiler_params=pltpu.CompilerParams(
            collective_id=0, has_side_effects=True,
            vmem_limit_bytes=60 * 2**20
        ),
    )(
        *lookup_tables(table),
        queries.reshape(total_rows, COLS),
        keys,
        values,
        out_weight,
    )
    return projected.reshape(BLOCKS, ROWS, out_weight.shape[1])


def solution(mesh):
    placed = (
        P("dp", None, "tensor"),
        P("dp", None, "tensor"),
        P("dp", None, "tensor"),
        P(None, "tensor"),
        P("dp"),
        P("dp", None),
        P("dp", None),
        P("dp", None),
    )
    return jax.shard_map(
        body, mesh=mesh, in_specs=placed, out_specs=P("dp", None, "tensor"), check_vma=False
    )
```
